256 devices in a mesh: row: 16 (over x_hi, z), col: 8 (over x_lo, y), rep: 2 (over core).
Axes of the slice: x: 4 (x_hi: 2, x_lo: 2; x = x_hi * 2 + x_lo), y: 4, z: 8, core: 2. Of those that a mesh axis runs over, the one named last changes fastest.
Arguments:
- matrix: float32 [16384, 16384], P('row', 'col'), may hold values from -0.125 to 0.125
- vectors: float32 [64, 16384], P('rep', 'row'), may hold values from -0.3 to 0.3
Outputs:
- result: float32 [64, 16384], P('rep', 'row')
The draws below stay inside these ranges and needn't reach their ends.
All inputs are finite; a program needn't handle non-finite values.
Results may differ from the reference program's by a relative error of at most 0.00011.
Values sent between devices are 32-bit elements; how exact they have to be, the bound alone decides.
A program may use at most 64 MiB of HBM per device.

```python
import jax
import jax.numpy as jnp
from jax import lax

N = 16384
COLS = 64
TERMS = 6
STEPS = 1


def block_scale(rng, dims, split, smallest, largest):
    factor_of = 1.0
    for position, blocks in split:
        steps = jax.random.uniform(jax.random.fold_in(jax.random.fold_in(rng, 6), position), (blocks,), jnp.float32, smallest / len(split), largest / len(split))
        factor_of = factor_of * jnp.repeat(jnp.exp(steps), dims[position] // blocks).reshape((-1,) + (1,) * (len(dims) - 1 - position))
    return factor_of


def gaussian(stream_key, shape, deviation, limit, pieces=(), dtype=jnp.bfloat16):
    factor_of = block_scale(stream_key, shape, pieces, -0.22, 0.18) if pieces else 1.0
    entries = jax.random.normal(stream_key, shape, jnp.float32) * deviation * factor_of
    return jnp.minimum(jnp.maximum(entries, -limit), limit).astype(dtype)


def setup_inputs(seed: int = 0) -> dict:
    key_list = jax.random.split(jax.random.key(seed), 3)
    matrix = gaussian(key_list[0], (N, N), (N // 7) ** -0.5, 0.125, ((0, 16), (1, 8)), jnp.float32)
    vectors = gaussian(key_list[1], (COLS, N), 0.05, 0.3, ((0, 2), (1, 16)), jnp.float32)
    return {"matrix": matrix, "vectors": vectors}


def reference(matrix, vectors):
    current = vectors
    for section in range(STEPS):
        summand = current
        running = current
        for degree in range(1, TERMS + 1):
            product = lax.dot_general(summand, matrix, (((1,), (1,)), ((), ())), precision=lax.Precision.HIGHEST, preferred_element_type=jnp.float32)
            summand = product / float(degree * STEPS)
            running = running + summand
        current = running
    return current
```

```python
import functools

import jax
import jax.numpy as jnp
from jax import lax
from jax.experimental import pallas as pl
from jax.experimental.pallas import tpu as pltpu
from jax.sharding import PartitionSpec as P

TERMS = 6
STEPS = 1
MESH = pl.DeviceIdType.MESH
BF16 = jnp.bfloat16
F32 = jnp.float32
LANES = 128
ORDER = (4, 3, 5, 2, 6, 1, 7, 0)


def halves(value):
    high = value.astype(BF16)
    return high, (value - high.astype(F32)).astype(BF16)


def kernel(
    rows, cols, mat_ref, vec_ref, out_ref,
    stage, a_high, a_low, operand, xin, part, arrived, total, final, running,
    load_sem, x_send, x_recv, p_send, p_recv, f_send, f_recv,
):
    r, c = lax.axis_index("row"), lax.axis_index("col")
    blocks = rows // cols
    pieces = blocks * cols
    height = vec_ref.shape[0]
    home = lax.div(r, blocks)
    slot = lax.rem(r, blocks) * cols + c
    mine = home == c
    half, ring = rows // 8, 8
    chunks = stage.shape[0]
    depth = stage.shape[1]

    loads = [
        pltpu.make_async_copy(mat_ref.at[pl.ds(n * depth, depth), :], stage.at[n], load_sem.at[n])
        for n in range(chunks)
    ]
    for load in loads:
        load.start()

    barrier = pltpu.get_barrier_semaphore()
    for step in range(1, cols):
        pl.semaphore_signal(
            barrier, inc=1, device_id={"col": lax.rem(c + step, cols)}, device_id_type=MESH
        )
    for block in range(blocks):
        for k in range(cols):
            source = c * blocks + block
            itself = jnp.logical_and(source == r, c == k)

            @pl.when(jnp.logical_not(itself))
            def _():
                pl.semaphore_signal(
                    barrier, inc=1, device_id={"row": source, "col": k}, device_id_type=MESH
                )

    total[0] = vec_ref[:, pl.ds(pl.multiple_of(c * LANES, LANES), LANES)]
    running[...] = total[0]

    @pl.when(mine)
    def _():
        pl.semaphore_wait(barrier, cols - 1 + rows - 1)

    @pl.when(jnp.logical_not(mine))
    def _():
        pl.semaphore_wait(barrier, cols - 1 + rows)

    z, hi = lax.rem(r, ring), lax.div(r, ring)

    def spread(degree):
        for step in ORDER:
            for side in range(half):
                target = lax.rem(hi + 1 + side, half) * ring + lax.rem(z + step, ring)
                copy = pltpu.make_async_remote_copy(
                    src_ref=total.at[degree],
                    dst_ref=xin.at[degree, slot],
                    send_sem=x_send.at[degree],
                    recv_sem=x_recv.at[degree, slot],
                    device_id={"row": target, "col": home},
                    device_id_type=MESH,
                )
                if step == 0 and side == half - 1:
                    pl.when(jnp.logical_not(mine))(copy.start)

                    @pl.when(mine)
                    def _():
                        xin[degree, slot] = total[degree]
                else:
                    copy.start()

    def sent(degree):
        count = pl.ds(0, rows - 1)

        @pl.when(mine)
        def _():
            pltpu.make_async_copy(
                xin.at[degree, count], xin.at[degree, count], x_send.at[degree]
            ).wait()

        @pl.when(jnp.logical_not(mine))
        def _():
            pltpu.make_async_copy(xin.at[degree], xin.at[degree], x_send.at[degree]).wait()

    spread(0)

    for n in range(chunks):
        loads[n].wait()
        high, low = halves(stage[n])
        a_high[n * depth : (n + 1) * depth] = high
        a_low[n * depth : (n + 1) * depth] = low

    wide = 2 * LANES

    def one_degree(degree, carry):
        for p in range(pieces):
            itself = jnp.logical_and(mine, slot == p)

            @pl.when(jnp.logical_not(itself))
            def _():
                pltpu.make_async_copy(
                    xin.at[degree, p], xin.at[degree, p], x_recv.at[degree, p]
                ).wait()

            high, low = halves(xin[degree, p])
            operand[0:height, p * LANES : (p + 1) * LANES] = high
            operand[height : 2 * height, p * LANES : (p + 1) * LANES] = low
        for step in range(1, cols // 2 + 1):
            pair = lax.rem(lax.div(c, 2) + step, cols // 2)
            window = pl.ds(pl.multiple_of(pair * wide, wide), wide)
            value = lax.dot_general(
                operand[...], a_high[window, :], (((1,), (1,)), ((), ())), preferred_element_type=F32
            )
            value += lax.dot_general(
                operand[...], a_low[window, :], (((1,), (1,)), ((), ())), preferred_element_type=F32
            )
            value = value[:height] + value[height:]
            for which in range(2):
                k = pair * 2 + which
                piece = value[:, which * LANES : (which + 1) * LANES]
                if step < cols // 2:
                    part[degree, k] = piece
                    pltpu.make_async_remote_copy(
                        src_ref=part.at[degree, k],
                        dst_ref=arrived.at[degree, c],
                        send_sem=p_send.at[degree],
                        recv_sem=p_recv.at[degree],
                        device_id={"col": k},
                        device_id_type=MESH,
                    ).start()
                else:
                    part[degree, k] = piece

                    @pl.when(k != c)
                    def _():
                        pltpu.make_async_remote_copy(
                            src_ref=part.at[degree, k],
                            dst_ref=arrived.at[degree, c],
                            send_sem=p_send.at[degree],
                            recv_sem=p_recv.at[degree],
                            device_id={"col": k},
                            device_id_type=MESH,
                        ).start()

        others = pl.ds(0, cols - 1)
        pltpu.make_async_copy(
            arrived.at[degree, others], arrived.at[degree, others], p_recv.at[degree]
        ).wait()
        arrived[degree, c] = part[degree, c]
        summed = arrived[degree, 0]
        for k in range(1, cols):
            summed = summed + arrived[degree, k]
        summed = summed / ((degree + 1) * STEPS).astype(F32)
        running[...] += summed

        @pl.when(degree < TERMS - 1)
        def _():
            total[degree + 1] = summed
            spread(degree + 1)

        sent(degree)
        pltpu.make_async_copy(
            arrived.at[degree, others], arrived.at[degree, others], p_send.at[degree]
        ).wait()
        return carry

    lax.fori_loop(0, TERMS, one_degree, 0)

    for step in range(1, cols):
        pltpu.make_async_remote_copy(
            src_ref=running,
            dst_ref=final.at[c],
            send_sem=f_send,
            recv_sem=f_recv,
            device_id={"col": lax.rem(c + step, cols)},
            device_id_type=MESH,
        ).start()
    others = pl.ds(0, cols - 1)
    pltpu.make_async_copy(final.at[others], final.at[others], f_recv).wait()
    final[c] = running[...]
    for k in range(cols):
        out_ref[:, k * LANES : (k + 1) * LANES] = final[k]
    pltpu.make_async_copy(final.at[others], final.at[others], f_send).wait()


def local(rows, cols, matrix, vectors):
    height, width = vectors.shape
    tall, deep = matrix.shape
    pieces = rows // cols * cols
    chunks = 8
    return pl.pallas_call(
        functools.partial(kernel, rows, cols),
        out_shape=jax.ShapeDtypeStruct(vectors.shape, F32),
        in_specs=[
            pl.BlockSpec(memory_space=pl.ANY),
            pl.BlockSpec(memory_space=pltpu.VMEM),
        ],
        out_specs=pl.BlockSpec(memory_space=pltpu.VMEM),
        scratch_shapes=[
            pltpu.VMEM((chunks, tall // chunks, deep), F32),
            pltpu.VMEM((tall, deep), BF16),
            pltpu.VMEM((tall, deep), BF16),
            pltpu.VMEM((2 * height, deep), BF16),
            pltpu.VMEM((TERMS, pieces, height, LANES), F32),
            pltpu.VMEM((TERMS, cols, height, LANES), F32),
            pltpu.VMEM((TERMS, cols, height, LANES), F32),
            pltpu.VMEM((TERMS, height, LANES), F32),
            pltpu.VMEM((cols, height, LANES), F32),
            pltpu.VMEM((height, LANES), F32),
            pltpu.SemaphoreType.DMA((chunks,)),
            pltpu.SemaphoreType.DMA((TERMS,)),
            pltpu.SemaphoreType.DMA((TERMS, pieces)),
            pltpu.SemaphoreType.DMA((TERMS,)),
            pltpu.SemaphoreType.DMA((TERMS,)),
            pltpu.SemaphoreType.DMA,
            pltpu.SemaphoreType.DMA,
        ],
        compiler_params=pltpu.CompilerParams(
            collective_id=0, has_side_effects=True, vmem_limit_bytes=60 * 2**20
        ),
    )(matrix, vectors)


def solution(mesh):
    rows, cols = mesh.shape["row"], mesh.shape["col"]
    return jax.shard_map(
        functools.partial(local, rows, cols),
        mesh=mesh,
        in_specs=(P("row", "col"), P("rep", "row")),
        out_specs=P("rep", "row"),
        check_vma=False,
    )
```
